512 devices in a mesh: tm: 32 (over z, x), space: 16 (over y, core).
Axes of the slice: x: 4, y: 8, z: 8, core: 2. Of those that a mesh axis runs over, the one named last changes fastest.
Arguments:
- snapshots: bfloat16 [4096, 73728], P('tm', 'space'), may hold values from -12 to 12
- start_block: float32 [4096, 20], P('tm'), may hold values from -6 to 6
- merge_mix: float32 [40, 20], replicated, may hold values from -1 to 1
Outputs:
- modes: float32 [20, 73728], P(None, ('space', 'tm'))
- spectrum: float32 [20], replicated
The draws below stay inside these ranges and needn't reach their ends.
All inputs are finite; a program needn't handle non-finite values.
Results may differ from the reference program's by a relative error of at most 0.012.
Values sent between devices are 32-bit elements; how exact they have to be, the bound alone decides.
A program may use at most 64 MiB of HBM per device.

```python
import math
import jax
import jax.numpy as jnp
from jax import lax

R = 20
SNAP_DEV = 128
WIDTH = 73728
ITERS = 2
LEVELS = 5
SNAPSHOTS = 4096
N_TM = 32


def draw_snapshots(key, part):
    keys = jax.random.split(jax.random.fold_in(key, 7), 3)
    steps = jnp.arange(R, dtype=jnp.float32)
    shared_decay = 0.95 ** steps
    own_decay = 0.7 * 0.95 ** steps
    shared_shapes = jax.random.normal(keys[0], (R, WIDTH), jnp.float32)
    rough = jnp.exp(jax.random.uniform(keys[1], (1, WIDTH), jnp.float32, math.log(0.7), math.log(1.4)))
    ramp = jnp.exp(jnp.linspace(math.log(0.5), math.log(2.0), WIDTH, dtype=jnp.float32))[None, :]
    col_scale = ramp * rough

    def one_tile(index):
        tile_keys = jax.random.split(jax.random.fold_in(keys[2], index), 4)
        shared_w = jax.random.normal(tile_keys[0], (SNAP_DEV, R), jnp.float32) * shared_decay
        own_w = jax.random.normal(tile_keys[1], (SNAP_DEV, R), jnp.float32) * own_decay
        own_shapes = jax.random.normal(tile_keys[2], (R, WIDTH), jnp.float32)
        noise = jax.random.normal(tile_keys[3], (SNAP_DEV, WIDTH), jnp.float32)
        values = jnp.dot(shared_w, shared_shapes, precision=lax.Precision.HIGHEST)
        values = values + jnp.dot(own_w, own_shapes, precision=lax.Precision.HIGHEST) + 0.1 * noise
        values = values * col_scale
        return jnp.clip(values, -12.0, 12.0).astype(jnp.bfloat16)
    tiles = lax.map(one_tile, jnp.arange(SNAPSHOTS // SNAP_DEV, dtype=jnp.int32))
    return tiles.reshape(SNAPSHOTS, WIDTH)


def levels(stream_key, extent, cuts, least, top_value):
    def one(axis_at, shards_of):
        steps = jax.random.uniform(jax.random.fold_in(jax.random.fold_in(stream_key, 6), axis_at), (shards_of,), jnp.float32, least / len(cuts), top_value / len(cuts))
        return jnp.repeat(jnp.exp(steps), extent[axis_at] // shards_of).reshape((-1,) + (1,) * (len(extent) - axis_at - 1))

    loudness = one(*cuts[0])
    for cut in cuts[1:]:
        loudness = loudness * one(*cut)
    return loudness


def centred(own_key, extent, deviation, limit, cuts=(), held_as=jnp.bfloat16):
    array = deviation * jax.random.normal(own_key, extent, jnp.float32)
    if cuts:
        array = array * levels(own_key, extent, cuts, -0.22, 0.18)
    return jnp.clip(array, -limit, limit).astype(held_as)


def setup_inputs(seed: int = 0) -> dict:
    key_list = jax.random.split(jax.random.key(seed), 4)
    snapshots = draw_snapshots(jax.random.fold_in(key_list[3], 71), 0)
    start_block = centred(key_list[1], (SNAPSHOTS, R), 1.0, 6.0, ((0, 32),), jnp.float32)
    merge_mix = centred(key_list[2], (2 * R, R), (2 * R) ** -0.5, 1.0, (), jnp.float32)
    return {"snapshots": snapshots, "start_block": start_block, "merge_mix": merge_mix}


HIGHEST_PREC = lax.Precision.HIGHEST

def merge_rule(gram_mat, mixing):
    weighted = jnp.dot(gram_mat, mixing, precision=HIGHEST_PREC)
    small_gram = jnp.dot(mixing.T, weighted, precision=HIGHEST_PREC)
    cholesky_low = jnp.linalg.cholesky(small_gram)
    coef_map = jax.scipy.linalg.solve_triangular(cholesky_low, mixing.T, lower=True)
    spread = jnp.dot(coef_map, gram_mat, precision=HIGHEST_PREC)
    singular = jnp.sqrt(lax.optimization_barrier(jnp.sum(spread * spread, axis=1)))
    return (coef_map, singular)

def tile_factor(window, start):
    block_proj = start
    for rounds in range(ITERS):
        rounded = block_proj.astype(jnp.bfloat16)
        images = jnp.dot(rounded.T.astype(jnp.float32), window.astype(jnp.float32), preferred_element_type=jnp.float32)
        images_b = images.astype(jnp.bfloat16)
        gram_mat = jnp.dot(images_b.astype(jnp.float32), images_b.T.astype(jnp.float32), preferred_element_type=jnp.float32)
        projected = jnp.dot(window.astype(jnp.float32), images_b.T.astype(jnp.float32), preferred_element_type=jnp.float32)
        cholesky_low = jnp.linalg.cholesky(gram_mat)
        block_proj = jax.scipy.linalg.solve_triangular(cholesky_low, projected.T, lower=True).T
    singular = jnp.sqrt(lax.optimization_barrier(jnp.sum(block_proj * block_proj, axis=0)))
    basis_rows = jax.scipy.linalg.solve_triangular(cholesky_low, images_b.astype(jnp.float32), lower=True)
    return singular[:, None] * basis_rows

def reference(snapshots, start_block, merge_mix):
    windows = snapshots.reshape(N_TM, SNAP_DEV, WIDTH)
    starts = start_block.reshape(N_TM, SNAP_DEV, R)
    factors = lax.map(lambda pieces: tile_factor(pieces[0], pieces[1]), (windows, starts))
    for height in range(LEVELS):
        pair_count = factors.shape[0] // 2
        stacked = factors.reshape(pair_count, 2 * R, WIDTH)
        gram_mat = jnp.einsum('gam,gbm->gab', stacked, stacked, precision=HIGHEST_PREC)
        coef_map, singular = jax.vmap(merge_rule, in_axes=(0, None))(gram_mat, merge_mix)
        basis_rows = jnp.einsum('grk,gkm->grm', coef_map, stacked, precision=HIGHEST_PREC)
        factors = singular[:, :, None] * basis_rows
    modes = basis_rows[0] * math.sqrt(WIDTH)
    spectrum = singular[0] / math.sqrt(SNAP_DEV * WIDTH)
    return (modes, spectrum)
```

```python
import functools
import math

import jax
import jax.numpy as jnp
from jax import lax
from jax.experimental import pallas as pl
from jax.experimental.pallas import tpu as pltpu
from jax.sharding import PartitionSpec as P

MESH = pl.DeviceIdType.MESH
HIGH = lax.Precision.HIGHEST
F32 = jnp.float32
BF16 = jnp.bfloat16
R = 20
RP = 24
N_SPACE = 16
N_TM = 32
G1 = 8
G2 = 4
PIECE = 144
LOCAL = 4608
X_PARTS = 4
ITERS = 2
S_A, S_C, X1, A1, B1, C1, X2, A2, B2, C2 = range(10)


def dot(a, b):
    return lax.dot_general(a, b, (((1,), (0,)), ((), ())), precision=HIGH, preferred_element_type=F32)


def dot_t(a, b):
    return lax.dot_general(a, b, (((1,), (1,)), ((), ())), precision=HIGH, preferred_element_type=F32)


def roll(x, by, axis=-1):
    size = x.shape[axis]
    by = by % size
    return x if by == 0 else pltpu.roll(x, by, axis % x.ndim)


def iota(shape, axis):
    return lax.broadcasted_iota(jnp.int32, shape, axis)


def keep_lanes(x, low, high):
    lane = iota(x.shape, x.ndim - 1)
    return jnp.where((lane >= low) & (lane < high), x, 0.0)


def gram_columns(rows, vectors):
    return [jnp.sum(rows * vectors[..., k : k + 1, :], axis=-1, keepdims=True) for k in range(R)]


def eliminate(columns, augmented):
    columns = list(columns)
    augmented = list(augmented)
    row_c = iota(columns[0].shape, columns[0].ndim - 2)
    row_a = iota(augmented[0].shape, augmented[0].ndim - 2)
    for j in range(R):
        inv = lax.rsqrt(columns[j][..., j : j + 1, :])
        low = jnp.where(row_c > j, columns[j] * inv, 0.0)
        for k in range(j + 1, R):
            columns[k] = columns[k] - low * low[..., k : k + 1, :]
        for n, a in enumerate(augmented):
            top = a[..., j : j + 1, :] * inv
            augmented[n] = jnp.where(row_a == j, top, a - low * top)
    return augmented


def combine(wide, first, second):
    total = None
    for k in range(R):
        for block, at in ((first, k), (second, R + k)):
            term = wide[at] * block[..., k : k + 1, :]
            total = term if total is None else total + term
    return total


def merge(cross, cross_t, square_a, square_b, mix_t, wide, images):
    lane, row = iota((1, RP, 128), 2), iota((1, RP, 128), 1)
    top = jnp.where(lane == row, square_a, 0.0) + roll(cross, R)
    bottom = cross_t + jnp.where(lane == row + R, square_b, 0.0)
    weighted = combine(wide, top, bottom)
    done = eliminate(gram_columns(weighted, mix_t[None]), [weighted] + images)
    squares = jnp.sum(done[0] * done[0], axis=-1, keepdims=True)
    return done[1:], squares


def pack_first(gram):
    lane = iota((40, 256), 1)
    row = iota((40, 256), 0)
    out = []
    for half in range(2):
        mine = gram[40 * half : 40 * half + 40]
        other = gram[80 * half : 80 * half + 40]
        far = keep_lanes(roll(mine, -80), 0, 80)
        near = keep_lanes(roll(other, 40 - 80 * half), 80, 120)
        total = far + near
        for q in range(2):
            p = 2 * q + half
            block = gram[40 * p : 40 * p + 40]
            norm = jnp.sum(jnp.where(lane == row + 40 * p, block, 0.0), axis=1, keepdims=True)
            total = total + jnp.where(lane == 120 + q, norm, 0.0)
        out.append(total[:, :128])
    last = None
    for p in range(4):
        block = roll(gram[40 * p : 40 * p + RP], -R - R * p)
        block = keep_lanes(block, R * p, R * p + R)
        last = block if last is None else last + block
    out.append(jnp.where(iota((RP, 128), 0) < R, last[:, :128], 0.0))
    return jnp.concatenate(out, axis=0)


def small(x):
    keep = (iota(x.shape, x.ndim - 1) < R) & (iota(x.shape, x.ndim - 2) < R)
    return jnp.where(keep, x, 0.0)


def transposed(x):
    full = jnp.concatenate([x, jnp.zeros((128 - RP, 128), F32)], axis=0)
    return full.T[:RP]


def tall(x):
    return jnp.concatenate([x, jnp.zeros((128 - RP, 128), F32)], axis=0)


def pair_up(maps, squares, blocks, width, mix_t, wide, last=False):
    crosses, crosses_t, images = [], [], []
    for p, block in enumerate(blocks):
        a, b = maps[2 * p], maps[2 * p + 1]
        mid = keep_lanes(dot(a[:, :width], block), 0, width)
        crosses.append(small(dot_t(mid, tall(b))))
        crosses_t.append(small(dot_t(b, tall(mid))))
        images.append((dot(mix_t[:, :RP], a), dot(roll(mix_t, -R)[:, :RP], b)))
    stack = lambda seq: jnp.stack(seq, axis=0)
    if 2 * width <= 128:
        carried = [stack([x + roll(y, width) for x, y in images])]
    else:
        carried = [stack([x for x, _ in images]), stack([y for _, y in images])]
    sq_a = stack([squares[2 * p] for p in range(len(blocks))])
    sq_b = stack([squares[2 * p + 1] for p in range(len(blocks))])
    out, sq = merge(stack(crosses), stack(crosses_t), sq_a, sq_b, mix_t, wide, carried)
    if not last:
        scale = jnp.sqrt(sq)
        out = [x * scale for x in out]
    return out, sq


def base_level(crosses, norms, mix_t, wide):
    stack = lambda seq: jnp.stack(seq, axis=0)
    cross = stack(crosses)
    cross_t = stack([transposed(c) for c in crosses])
    images = jnp.broadcast_to(mix_t[None], cross.shape)
    out, sq = merge(cross, cross_t, stack(norms[0::2]), stack(norms[1::2]), mix_t, wide, [images])
    return out[0] * jnp.sqrt(sq), sq


def rows_of(squares):
    return jnp.where(iota(squares.shape, squares.ndim - 2) < R, squares, 0.0)


def first_stage(summed, norm_rows, mix_t, wide):
    last = summed[80 : 80 + RP]
    crosses = [small(roll(last, -R * p)) for p in range(4)]
    norms = [rows_of(norm_rows(R * (t % 4), 120 + t // 4)) for t in range(8)]
    maps, sq = base_level(crosses, norms, mix_t, wide)
    near = roll(summed[:80], -80)
    out, sq2 = pair_up([maps[p] for p in range(4)], [sq[p] for p in range(4)], [near[0:40], near[40:80]], 40, mix_t, wide)
    out, sq3 = pair_up([out[0][0], out[0][1]], [sq2[0], sq2[1]], [summed[0:80]], 80, mix_t, wide)
    return out[0][0], out[1][0]


def pack_second(gram):
    far = keep_lanes(roll(gram[0:40], -40), 0, 40)
    lane, row = iota((40, 128), 1), iota((40, 128), 0)
    total = far
    for p in range(2):
        block = gram[40 * p : 40 * p + 40]
        norm = jnp.sum(jnp.where(lane == row + 40 * p, block, 0.0), axis=1, keepdims=True)
        total = total + jnp.where(lane == 80 + p, norm, 0.0)
        near = keep_lanes(roll(block, 40 + R * p - 40 * p - R), 40 + R * p, 60 + R * p)
        total = total + jnp.where(row < R, near, 0.0)
    return total


def second_stage(summed, norm_rows, mix_t, wide):
    top = summed[0:RP]
    crosses = [small(roll(top, -40 - R * p)) for p in range(2)]
    norms = [rows_of(norm_rows(R * (t % 2), 80 + t // 2)) for t in range(4)]
    maps, sq = base_level(crosses, norms, mix_t, wide)
    out, sq2 = pair_up([maps[0], maps[1]], [sq[0], sq[1]], [summed[0:40]], 40, mix_t, wide, last=True)
    return out[0][0], sq2[0]


def first_pieces(factor):
    lane = iota((RP, 128), 1)
    for place in range(G1):
        windows = []
        for g in range(G2):
            at = 128 * (9 * g + place)
            windows.append(roll(factor(at), 16 * g - 16 * place))
        tiles = [windows[0][:, :128]]
        for g in range(1, G2):
            tiles.append(jnp.where(lane < 16 * g, windows[g - 1][:, 128:], windows[g][:, :128]))
        tiles.append(jnp.where(lane < 64, windows[3][:, 128:], 0.0))
        yield place, tiles


def split3(x):
    high = x.astype(BF16)
    rest = x - high.astype(F32)
    mid = rest.astype(BF16)
    low = (rest - mid.astype(F32)).astype(BF16)
    return high, mid, low


def tile_step(o_t, s_mat, extra):
    proj = dot(o_t, s_mat)
    return eliminate(gram_columns(proj, o_t), [proj] + extra)


def kernel(x_hbm, start_ref, mix_ref, modes_ref, spec_ref,
           xv, square, wide_ref, factor_ref, part_s, got_s, sum_s,
           out1, in1, slab1, part1, got1, mid1, sum1,
           wide2, out2, in2, slab2, part2, got2, mid2, sum2,
           load_sem, send_sem, recv_sem):
    tm = lax.axis_index("tm")
    sp = lax.axis_index("space")
    group, place = tm // G1, lax.rem(tm, G1)
    own_tile = sp // 2 + 8 * (1 - lax.rem(sp, 2))

    cols = LOCAL // X_PARTS
    loads = [
        pltpu.make_async_copy(x_hbm.at[:, pl.ds(cols * c, cols)], xv.at[:, pl.ds(cols * c, cols)], load_sem.at[c])
        for c in range(X_PARTS)
    ]
    for load in loads:
        load.start()

    barrier = pltpu.get_barrier_semaphore()

    def greet_space(d, carry):
        pl.semaphore_signal(barrier, inc=1, device_id=(tm, lax.rem(sp + d, N_SPACE)), device_id_type=MESH)
        return carry

    def greet_tm(d, carry):
        pl.semaphore_signal(barrier, inc=1, device_id=(lax.rem(tm + d, N_TM), sp), device_id_type=MESH)
        return carry

    lax.fori_loop(1, N_SPACE, greet_space, 0)
    lax.fori_loop(1, N_TM, greet_tm, 0)

    square[...] = jnp.zeros((128, 128), F32)
    square[:, 0:R] = start_ref[...]
    o_t = square[...].T[0:RP].astype(BF16).astype(F32)
    square[...] = jnp.zeros((128, 128), F32)
    square[0 : 2 * R, 0:R] = mix_ref[...]
    mix_t = square[...].T[0:RP]
    for k in range(2 * R):
        wide_ref[k] = jnp.broadcast_to(mix_t[:, k : k + 1], (RP, 128))
    slab1[...] = jnp.zeros(slab1.shape, F32)
    slab2[...] = jnp.zeros(slab2.shape, F32)
    wide = [wide_ref.at[k] for k in range(2 * R)]

    s_mat = jnp.zeros((128, 128), F32)
    for c in range(X_PARTS):
        loads[c].wait()
        block = xv[:, cols * c : cols * (c + 1)]
        s_mat = s_mat + lax.dot_general(block, block, (((1,), (1,)), ((), ())), preferred_element_type=F32)
    part_s[...] = s_mat.reshape(16, 8, 128)

    pl.semaphore_wait(barrier, N_SPACE - 1 + N_TM - 1)

    def rounds(first, last, make):
        def go(d, carry):
            make(d, lambda copy: copy.start())
            return carry

        def end(d, carry):
            make(d, lambda copy: copy.wait_send())
            return carry

        return lambda: lax.fori_loop(first, last, go, 0), lambda: lax.fori_loop(first, last, end, 0)

    def arrived(ref, count, phase):
        some = ref.at[pl.ds(0, count)]
        pltpu.make_async_copy(some, some, recv_sem.at[phase]).wait()

    def send(src, dst, d, phase, tm_to, sp_to):
        return pltpu.make_async_remote_copy(
            src_ref=src, dst_ref=dst, send_sem=send_sem.at[d], recv_sem=recv_sem.at[phase],
            device_id=(tm_to, sp_to), device_id_type=MESH)

    def all_reduce(part, got, mid, total, tiles, phases, tm_count, tm_place, tm_peer):
        phase_a, phase_b, phase_c = phases

        def scatter(d, act):
            peer = lax.rem(sp + d, N_SPACE)
            tile = peer // 2 + 8 * (1 - lax.rem(peer, 2))

            @pl.when(tile < tiles)
            def _():
                act(send(part.at[tile], got.at[sp], d, phase_a, tm, peer))

        def across(d, act):
            act(send(mid.at[tm_place], mid.at[tm_place], d, phase_b, tm_peer(d), sp))

        def gather(d, act):
            act(send(total.at[own_tile], total.at[own_tile], d, phase_c, tm, lax.rem(sp + d, N_SPACE)))

        go, end = rounds(1, N_SPACE, scatter)
        go()

        @pl.when(own_tile < tiles)
        def _():
            got[sp] = part[own_tile]
            arrived(got, N_SPACE - 1, phase_a)
            acc = jnp.sum(got[...], axis=0)
            end()
            if tm_count > 1:
                mid[tm_place] = acc
                go_b, end_b = rounds(1, tm_count, across)
                go_b()
                arrived(mid, tm_count - 1, phase_b)
                acc = jnp.sum(mid[...], axis=0)
                end_b()
            total[own_tile] = acc
            go_c, end_c = rounds(1, N_SPACE, gather)
            go_c()
            arrived(total, tiles - 1, phase_c)
            end_c()

        @pl.when(own_tile >= tiles)
        def _():
            end()
            arrived(total, tiles, phase_c)

    all_reduce(part_s, got_s, None, sum_s, 16, (S_A, None, S_C), 1, None, None)
    s_mat = sum_s[...].reshape(128, 128)

    eye = jnp.where(iota((RP, 128), 0) == iota((RP, 128), 1), 1.0, 0.0)
    for step in range(ITERS):
        if step:
            o_t = o_t.astype(BF16).astype(F32)
        last_block = o_t
        o_t, *inverse = tile_step(o_t, s_mat, [eye] if step == ITERS - 1 else [])
    scale = jnp.sqrt(jnp.sum(o_t * o_t, axis=1, keepdims=True))
    weights = jnp.concatenate(split3(jnp.concatenate([inverse[0] * scale, jnp.zeros((32 - RP, 128), F32)], axis=0)[:, :32]), axis=0)
    block = jnp.concatenate([last_block, jnp.zeros((32 - RP, 128), F32)], axis=0).astype(BF16)
    for c in range(X_PARTS):
        at = slice(cols * c, cols * (c + 1))
        image = jnp.dot(block, xv[:, at], preferred_element_type=F32).astype(BF16)
        three = jnp.dot(weights, image, preferred_element_type=F32)
        factor_ref[:, at] = (three[0:RP] + three[32 : 32 + RP]) + three[64 : 64 + RP]

    for there, tiles in first_pieces(lambda at: factor_ref[:, at : at + 256]):
        for c, t in enumerate(tiles):
            out1[there, :, 128 * c : 128 * (c + 1)] = t[0:R]

    def exchange1(d, act):
        there = lax.rem(place + d, G1)
        act(send(out1.at[there], in1.at[place], d, X1, G1 * group + there, sp))

    go, end = rounds(1, G1, exchange1)
    go()
    in1[place] = out1[place]
    arrived(in1, G1 - 1, X1)
    end()
    for t in range(G1):
        slab1[R * t : R * t + R, :] = in1[t]
    rows = slab1[0 : R * G1]
    gram = dot_t(rows, slab1[...])
    part1[...] = jnp.concatenate([pack_first(gram), jnp.zeros((24, 128), F32)], axis=0).reshape(16, 8, 128)
    all_reduce(part1, got1, mid1, sum1, 13, (A1, B1, C1), G1, place, lambda d: G1 * group + lax.rem(place + d, G1))
    square[0:104] = sum1[0:13].reshape(104, 128)
    left, right = first_stage(square[...], lambda row, lane: square[row : row + RP, :][:, lane : lane + 1], mix_t, wide_ref[...])
    merged = dot(left[:, :80], slab1[0:80]) + dot(right[:, :80], slab1[80:160])
    wide2[...] = merged

    for g in range(G2):
        window = keep_lanes(roll(wide2[:, 128 * g : 128 * g + 256], -16 * g), 0, PIECE)
        out2[g] = window[0:R]

    def exchange2(d, act):
        there = lax.rem(group + d, G2)
        act(send(out2.at[there], in2.at[group], d, X2, G1 * there + place, sp))

    go, end = rounds(1, G2, exchange2)
    go()
    in2[group] = out2[group]
    arrived(in2, G2 - 1, X2)
    end()
    for t in range(G2):
        slab2[R * t : R * t + R, :] = in2[t]
    gram = dot_t(slab2[0:80], slab2[...])
    part2[0:5] = pack_second(gram).reshape(5, 8, 128)
    all_reduce(part2, got2, mid2, sum2, 5, (A2, B2, C2), N_TM, tm, lambda d: lax.rem(tm + d, N_TM))
    square[0:40] = sum2[0:5].reshape(40, 128)
    coef, squares = second_stage(square[...], lambda row, lane: square[row : row + RP, :][:, lane : lane + 1], mix_t, wide_ref[...])
    final = dot(coef[:, :80], slab2[0:80]) * math.sqrt(LOCAL * N_SPACE)
    modes_ref[...] = final[0:R, 0:PIECE]
    values = jnp.sqrt(squares) * (1.0 / math.sqrt(128 * LOCAL * N_SPACE))
    spec_ref[...] = jnp.sum(eye * values, axis=0, keepdims=True)[:, 0:R]


def local(snapshots, start_block, merge_mix):
    vmem = pl.BlockSpec(memory_space=pltpu.VMEM)
    tile16 = pltpu.VMEM((16, 8, 128), F32)
    modes, spectrum = pl.pallas_call(
        kernel,
        out_shape=(jax.ShapeDtypeStruct((R, PIECE), F32), jax.ShapeDtypeStruct((1, R), F32)),
        in_specs=[pl.BlockSpec(memory_space=pl.ANY), vmem, vmem],
        out_specs=(vmem, vmem),
        scratch_shapes=[
            pltpu.VMEM((128, LOCAL), BF16),
            pltpu.VMEM((128, 128), F32),
            pltpu.VMEM((2 * R, RP, 128), F32),
            pltpu.VMEM((RP, LOCAL), F32),
            tile16, tile16, tile16,
            pltpu.VMEM((G1, R, 640), F32),
            pltpu.VMEM((G1, R, 640), F32),
            pltpu.VMEM((256, 640), F32),
            tile16, tile16, pltpu.VMEM((G1, 8, 128), F32), tile16,
            pltpu.VMEM((RP, 640), F32),
            pltpu.VMEM((G2, R, 256), F32),
            pltpu.VMEM((G2, R, 256), F32),
            pltpu.VMEM((128, 256), F32),
            tile16, tile16, pltpu.VMEM((N_TM, 8, 128), F32), tile16,
            pltpu.SemaphoreType.DMA((X_PARTS,)),
            pltpu.SemaphoreType.DMA((N_TM,)),
            pltpu.SemaphoreType.DMA((10,)),
        ],
        compiler_params=pltpu.CompilerParams(collective_id=0, has_side_effects=True),
    )(snapshots, start_block, merge_mix)
    return modes, spectrum.reshape(R)


def solution(mesh):
    return jax.shard_map(
        local,
        mesh=mesh,
        in_specs=(P("tm", "space"), P("tm", None), P()),
        out_specs=(P(None, ("space", "tm")), P()),
        check_vma=False,
    )
```

```python
import functools
import math

import jax
import jax.numpy as jnp
from jax import lax
from jax.experimental import pallas as pl
from jax.experimental.pallas import tpu as pltpu
from jax.sharding import PartitionSpec as P

MESH = pl.DeviceIdType.MESH
HIGH = lax.Precision.HIGHEST
F32 = jnp.float32
BF16 = jnp.bfloat16
R = 20
RP = 24
N_SPACE = 16
N_TM = 32
G1 = 8
G2 = 4
PIECE = 144
LOCAL = 4608
X_PARTS = 4
ITERS = 2
FAR8 = (4, 3, 5, 2, 6, 1, 7)
FAR_ZX = sorted(((dz, dx) for dz in range(8) for dx in range(4) if dz or dx), key=lambda d: -(min(d[0], 8 - d[0]) + min(d[1], 4 - d[1])))
FAR_GROUP = ((1, 2), (1, 1), (1, 3), (0, 2), (1, 0), (0, 1), (0, 3))
S_A, S_C, X1, A1, B1, C1, X2, A2, B2, C2 = range(10)


def dot(a, b):
    return lax.dot_general(a, b, (((1,), (0,)), ((), ())), precision=HIGH, preferred_element_type=F32)


def dot_t(a, b):
    return lax.dot_general(a, b, (((1,), (1,)), ((), ())), precision=HIGH, preferred_element_type=F32)


def roll(x, by, axis=-1):
    size = x.shape[axis]
    by = by % size
    return x if by == 0 else pltpu.roll(x, by, axis % x.ndim)


def iota(shape, axis):
    return lax.broadcasted_iota(jnp.int32, shape, axis)


def keep_lanes(x, low, high):
    lane = iota(x.shape, x.ndim - 1)
    return jnp.where((lane >= low) & (lane < high), x, 0.0)


def gram_columns(rows, vectors):
    return [
        jnp.sum(rows[..., k // 8 * 8 :, :] * vectors[..., k : k + 1, :], axis=-1, keepdims=True) for k in range(R)
    ]


def eliminate(columns, augmented):
    columns = list(columns)
    augmented = list(augmented)
    finished = [[] for _ in augmented]
    for j in range(R):
        start = j // 8 * 8
        if j and j == start:
            for n, a in enumerate(augmented):
                finished[n].append(a[..., :8, :])
                augmented[n] = a[..., 8:, :]
        here = columns[j]
        at = j - start
        inv = lax.rsqrt(here[..., at : at + 1, :])
        low = jnp.where(iota(here.shape, here.ndim - 2) > at, here * inv, 0.0)
        for k in range(j + 1, R):
            begin = k // 8 * 8
            columns[k] = columns[k] - low[..., begin - start :, :] * low[..., k - start : k - start + 1, :]
        for n, a in enumerate(augmented):
            top = a[..., at : at + 1, :] * inv
            augmented[n] = jnp.where(iota(a.shape, a.ndim - 2) == at, top, a - low * top)
    return [jnp.concatenate(done + [a], axis=-2) for done, a in zip(finished, augmented)]


def combine(wide, first, second):
    total = None
    for k in range(R):
        for block, at in ((first, k), (second, R + k)):
            term = wide[at] * block[..., k : k + 1, :]
            total = term if total is None else total + term
    return total


def merge(cross, cross_t, square_a, square_b, mix_t, wide, images):
    lane, row = iota((1, RP, 128), 2), iota((1, RP, 128), 1)
    top = jnp.where(lane == row, square_a, 0.0) + roll(cross, R)
    bottom = cross_t + jnp.where(lane == row + R, square_b, 0.0)
    weighted = combine(wide, top, bottom)
    done = eliminate(gram_columns(weighted, mix_t[None]), [weighted] + images)
    squares = jnp.sum(done[0] * done[0], axis=-1, keepdims=True)
    return done[1:], squares


def pack_first(gram):
    lane = iota((40, 256), 1)
    row = iota((40, 256), 0)
    out = []
    for half in range(2):
        mine = gram[40 * half : 40 * half + 40]
        other = gram[80 * half : 80 * half + 40]
        far = keep_lanes(roll(mine, -80), 0, 80)
        near = keep_lanes(roll(other, 40 - 80 * half), 80, 120)
        total = far + near
        for q in range(2):
            p = 2 * q + half
            block = gram[40 * p : 40 * p + 40]
            norm = jnp.sum(jnp.where(lane == row + 40 * p, block, 0.0), axis=1, keepdims=True)
            total = total + jnp.where(lane == 120 + q, norm, 0.0)
        out.append(total[:, :128])
    last = None
    for p in range(4):
        block = roll(gram[40 * p : 40 * p + RP], -R - R * p)
        block = keep_lanes(block, R * p, R * p + R)
        last = block if last is None else last + block
    out.append(jnp.where(iota((RP, 128), 0) < R, last[:, :128], 0.0))
    return jnp.concatenate(out, axis=0)


def small(x):
    keep = (iota(x.shape, x.ndim - 1) < R) & (iota(x.shape, x.ndim - 2) < R)
    return jnp.where(keep, x, 0.0)


def transposed(x):
    full = jnp.concatenate([x, jnp.zeros((128 - RP, 128), F32)], axis=0)
    return full.T[:RP]


def tall(x):
    return jnp.concatenate([x, jnp.zeros((128 - RP, 128), F32)], axis=0)


def pair_up(maps, squares, blocks, width, mix_t, wide, last=False):
    crosses, crosses_t, images = [], [], []
    for p, block in enumerate(blocks):
        a, b = maps[2 * p], maps[2 * p + 1]
        mid = keep_lanes(dot(a[:, :width], block), 0, width)
        crosses.append(small(dot_t(mid, tall(b))))
        crosses_t.append(small(dot_t(b, tall(mid))))
        images.append((dot(mix_t[:, :RP], a), dot(roll(mix_t, -R)[:, :RP], b)))
    stack = lambda seq: jnp.stack(seq, axis=0)
    if 2 * width <= 128:
        carried = [stack([x + roll(y, width) for x, y in images])]
    else:
        carried = [stack([x for x, _ in images]), stack([y for _, y in images])]
    sq_a = stack([squares[2 * p] for p in range(len(blocks))])
    sq_b = stack([squares[2 * p + 1] for p in range(len(blocks))])
    out, sq = merge(stack(crosses), stack(crosses_t), sq_a, sq_b, mix_t, wide, carried)
    if not last:
        scale = jnp.sqrt(sq)
        out = [x * scale for x in out]
    return out, sq


def base_level(crosses, norms, mix_t, wide):
    stack = lambda seq: jnp.stack(seq, axis=0)
    cross = stack(crosses)
    cross_t = stack([transposed(c) for c in crosses])
    images = jnp.broadcast_to(mix_t[None], cross.shape)
    out, sq = merge(cross, cross_t, stack(norms[0::2]), stack(norms[1::2]), mix_t, wide, [images])
    return out[0] * jnp.sqrt(sq), sq


def rows_of(squares):
    return jnp.where(iota(squares.shape, squares.ndim - 2) < R, squares, 0.0)


def first_stage(summed, norm_rows, mix_t, wide):
    last = summed[80 : 80 + RP]
    crosses = [small(roll(last, -R * p)) for p in range(4)]
    norms = [rows_of(norm_rows(R * (t % 4), 120 + t // 4)) for t in range(8)]
    maps, sq = base_level(crosses, norms, mix_t, wide)
    near = roll(summed[:80], -80)
    out, sq2 = pair_up([maps[p] for p in range(4)], [sq[p] for p in range(4)], [near[0:40], near[40:80]], 40, mix_t, wide)
    out, sq3 = pair_up([out[0][0], out[0][1]], [sq2[0], sq2[1]], [summed[0:80]], 80, mix_t, wide)
    return out[0][0], out[1][0]


def pack_second(gram):
    far = keep_lanes(roll(gram[0:40], -40), 0, 40)
    lane, row = iota((40, 128), 1), iota((40, 128), 0)
    total = far
    for p in range(2):
        block = gram[40 * p : 40 * p + 40]
        norm = jnp.sum(jnp.where(lane == row + 40 * p, block, 0.0), axis=1, keepdims=True)
        total = total + jnp.where(lane == 80 + p, norm, 0.0)
        near = keep_lanes(roll(block, 40 + R * p - 40 * p - R), 40 + R * p, 60 + R * p)
        total = total + jnp.where(row < R, near, 0.0)
    return total


def second_stage(summed, norm_rows, mix_t, wide):
    top = summed[0:RP]
    crosses = [small(roll(top, -40 - R * p)) for p in range(2)]
    norms = [rows_of(norm_rows(R * (t % 2), 80 + t // 2)) for t in range(4)]
    maps, sq = base_level(crosses, norms, mix_t, wide)
    out, sq2 = pair_up([maps[0], maps[1]], [sq[0], sq[1]], [summed[0:40]], 40, mix_t, wide, last=True)
    return out[0][0], sq2[0]


def first_pieces(factor):
    lane = iota((RP, 128), 1)
    for place in range(G1):
        windows = []
        for g in range(G2):
            at = 128 * (9 * g + place)
            windows.append(roll(factor(at), 16 * g - 16 * place))
        tiles = [windows[0][:, :128]]
        for g in range(1, G2):
            tiles.append(jnp.where(lane < 16 * g, windows[g - 1][:, 128:], windows[g][:, :128]))
        tiles.append(jnp.where(lane < 64, windows[3][:, 128:], 0.0))
        yield place, tiles


def split3(x):
    high = x.astype(BF16)
    rest = x - high.astype(F32)
    mid = rest.astype(BF16)
    low = (rest - mid.astype(F32)).astype(BF16)
    return high, mid, low


def tile_step(o_t, s_mat, extra):
    proj = dot(o_t, s_mat)
    return eliminate(gram_columns(proj, o_t), [proj] + extra)


def kernel(x_hbm, start_ref, mix_ref, out_ref,
           xv, square, wide_ref, factor_ref, part_s, got_s, sum_s,
           out1, in1, slab1, part1, got1, mid1, sum1,
           wide2, out2, in2, slab2, part2, got2, mid2, sum2,
           load_sem, send_sem, recv_sem):
    tm = lax.axis_index("tm")
    sp = lax.axis_index("space")
    group, place = tm // G1, lax.rem(tm, G1)
    y, core = sp // 2, lax.rem(sp, 2)
    z, x = tm // 4, lax.rem(tm, 4)

    cols = LOCAL // X_PARTS
    loads = [
        pltpu.make_async_copy(x_hbm.at[:, pl.ds(cols * c, cols)], xv.at[:, pl.ds(cols * c, cols)], load_sem.at[c])
        for c in range(X_PARTS)
    ]
    for load in loads:
        load.start()

    barrier = pltpu.get_barrier_semaphore()

    def greet_space(d, carry):
        pl.semaphore_signal(barrier, inc=1, device_id=(tm, lax.rem(sp + d, N_SPACE)), device_id_type=MESH)
        return carry

    def greet_tm(d, carry):
        pl.semaphore_signal(barrier, inc=1, device_id=(lax.rem(tm + d, N_TM), sp), device_id_type=MESH)
        return carry

    lax.fori_loop(1, N_SPACE, greet_space, 0)
    lax.fori_loop(1, N_TM, greet_tm, 0)

    square[...] = jnp.zeros((128, 128), F32)
    square[0:R] = start_ref[...]
    o_t = square[0:RP].astype(BF16).astype(F32)
    square[0:R] = jnp.zeros((R, 128), F32)
    square[0:R, 0 : 2 * R] = mix_ref[...]
    mix_t = square[0:RP]
    for k in range(2 * R):
        wide_ref[k] = jnp.broadcast_to(mix_t[:, k : k + 1], (RP, 128))
    slab1[...] = jnp.zeros(slab1.shape, F32)
    slab2[...] = jnp.zeros(slab2.shape, F32)
    wide = [wide_ref.at[k] for k in range(2 * R)]

    s_mat = jnp.zeros((128, 128), F32)
    for c in range(X_PARTS):
        loads[c].wait()
        block = xv[:, cols * c : cols * (c + 1)]
        s_mat = s_mat + lax.dot_general(block, block, (((1,), (1,)), ((), ())), preferred_element_type=F32)
    part_s[...] = s_mat.reshape(8, 16, 128)

    pl.semaphore_wait(barrier, N_SPACE - 1 + N_TM - 1)

    def start(copy):
        copy.start()

    def sent(copy):
        copy.wait_send()

    def arrived(ref, count, phase):
        some = ref.at[pl.ds(0, count)]
        pltpu.make_async_copy(some, some, recv_sem.at[phase]).wait()

    def send(src, dst, d, phase, tm_to, sp_to):
        return pltpu.make_async_remote_copy(
            src_ref=src, dst_ref=dst, send_sem=send_sem.at[d], recv_sem=recv_sem.at[phase],
            device_id=(tm_to, sp_to), device_id_type=MESH)

    def all_reduce(part, got, mid, total, phases, tm_place, tm_peers):
        phase_a, phase_b, phase_c = phases
        owners = part.shape[0]
        mine = (core == 1) & (y < owners)

        def scatter(act):
            for n, dy in enumerate(FAR8 + (0,)):
                to = lax.rem(y + dy, 8)

                @pl.when((to < owners) & (core == 0) if dy == 0 else to < owners)
                def _():
                    act(send(part.at[to], got.at[sp], n, phase_a, tm, 2 * to + 1))

        def across(act):
            for n, to in enumerate(tm_peers):
                act(send(mid.at[tm_place], mid.at[tm_place], n, phase_b, to, sp))

        def gather(act):
            for n, dy in enumerate(FAR8):
                for c in range(2):
                    act(send(total.at[y], total.at[y], 2 * n + c, phase_c, tm, 2 * lax.rem(y + dy, 8) + c))
            act(send(total.at[y], total.at[y], 14, phase_c, tm, 2 * y))

        scatter(start)

        @pl.when(mine)
        def _():
            got[sp] = part[y]
            arrived(got, N_SPACE - 1, phase_a)
            acc = jnp.sum(got[...], axis=0)
            if tm_peers:
                scatter(sent)
                mid[tm_place] = acc
                across(start)
                arrived(mid, len(tm_peers), phase_b)
                acc = jnp.sum(mid[...], axis=0)
                across(sent)
            total[y] = acc
            if not tm_peers:
                scatter(sent)
            gather(start)
            arrived(total, owners - 1, phase_c)
            gather(sent)

        @pl.when(jnp.logical_not(mine))
        def _():
            scatter(sent)
            arrived(total, owners, phase_c)

    all_reduce(part_s, got_s, None, sum_s, (S_A, None, S_C), None, ())
    s_mat = sum_s[...].reshape(128, 128)

    eye = jnp.where(iota((RP, 128), 0) == iota((RP, 128), 1), 1.0, 0.0)
    for step in range(ITERS):
        if step:
            o_t = o_t.astype(BF16).astype(F32)
        last_block = o_t
        o_t, *inverse = tile_step(o_t, s_mat, [eye] if step == ITERS - 1 else [])
    scale = jnp.sqrt(jnp.sum(o_t * o_t, axis=1, keepdims=True))
    weights = jnp.concatenate(split3(jnp.concatenate([inverse[0] * scale, jnp.zeros((32 - RP, 128), F32)], axis=0)[:, :32]), axis=0)
    block = jnp.concatenate([last_block, jnp.zeros((32 - RP, 128), F32)], axis=0).astype(BF16)
    for c in range(X_PARTS):
        at = slice(cols * c, cols * (c + 1))
        image = jnp.dot(block, xv[:, at], preferred_element_type=F32).astype(BF16)
        three = jnp.dot(weights, image, preferred_element_type=F32)
        factor_ref[:, at] = (three[0:RP] + three[32 : 32 + RP]) + three[64 : 64 + RP]

    for there, tiles in first_pieces(lambda at: factor_ref[:, at : at + 256]):
        for c, t in enumerate(tiles):
            out1[there, :, 128 * c : 128 * (c + 1)] = t[0:R]

    near = [lax.rem(place // 4 + dz, 2) * 4 + lax.rem(x + dx, 4) for dz, dx in FAR_GROUP]

    def exchange1(act):
        for n, there in enumerate(near):
            act(send(out1.at[there], in1.at[place], n, X1, G1 * group + there, sp))

    exchange1(start)
    in1[place] = out1[place]
    arrived(in1, G1 - 1, X1)
    exchange1(sent)
    for t in range(G1):
        slab1[R * t : R * t + R, :] = in1[t]
    rows = slab1[0 : R * G1]
    gram = dot_t(rows, slab1[...])
    part1[...] = jnp.concatenate([pack_first(gram), jnp.zeros((8, 128), F32)], axis=0).reshape(7, 16, 128)
    all_reduce(part1, got1, mid1, sum1, (A1, B1, C1), place, [G1 * group + there for there in near])
    square[0:112] = sum1[...].reshape(112, 128)
    left, right = first_stage(square[...], lambda row, lane: square[row : row + RP, :][:, lane : lane + 1], mix_t, wide_ref[...])
    merged = dot(left[:, :80], slab1[0:80]) + dot(right[:, :80], slab1[80:160])
    wide2[...] = merged

    for g in range(G2):
        window = keep_lanes(roll(wide2[:, 128 * g : 128 * g + 256], -16 * g), 0, PIECE)
        out2[g] = window[0:R]

    def exchange2(act):
        for n, dg in enumerate((2, 1, 3)):
            there = lax.rem(group + dg, G2)
            act(send(out2.at[there], in2.at[group], n, X2, G1 * there + place, sp))

    exchange2(start)
    in2[group] = out2[group]
    arrived(in2, G2 - 1, X2)
    exchange2(sent)
    for t in range(G2):
        slab2[R * t : R * t + R, :] = in2[t]
    gram = dot_t(slab2[0:80], slab2[...])
    part2[...] = pack_second(gram).reshape(5, 8, 128)
    everyone = [lax.rem(z + dz, 8) * 4 + lax.rem(x + dx, 4) for dz, dx in FAR_ZX]
    all_reduce(part2, got2, mid2, sum2, (A2, B2, C2), tm, everyone)
    square[0:40] = sum2[...].reshape(40, 128)
    coef, squares = second_stage(square[...], lambda row, lane: square[row : row + RP, :][:, lane : lane + 1], mix_t, wide_ref[...])
    final = dot(coef[:, :80], slab2[0:80]) * math.sqrt(LOCAL * N_SPACE)
    out_ref[0:RP] = final
    values = jnp.sqrt(squares) * (1.0 / math.sqrt(128 * LOCAL * N_SPACE))
    out_ref[RP : RP + 1, 0:128] = jnp.sum(eye * values, axis=0, keepdims=True)


def write_out(result_ref, modes_ref, spec_ref):
    modes_ref[...] = result_ref[0:R, 0:PIECE]
    spec_ref[...] = result_ref[RP : RP + 1, 0:R]


def local(snapshots, start_block, merge_mix):
    vmem = pl.BlockSpec(memory_space=pltpu.VMEM)
    pieces = lambda count, rows: pltpu.VMEM((count, rows, 128), F32)
    result = pl.pallas_call(
        kernel,
        out_shape=jax.ShapeDtypeStruct((32, 256), F32),
        in_specs=[pl.BlockSpec(memory_space=pl.ANY), vmem, vmem],
        out_specs=vmem,
        scratch_shapes=[
            pltpu.VMEM((128, LOCAL), BF16),
            pltpu.VMEM((128, 128), F32),
            pltpu.VMEM((2 * R, RP, 128), F32),
            pltpu.VMEM((RP, LOCAL), F32),
            pieces(8, 16), pieces(N_SPACE, 16), pieces(8, 16),
            pltpu.VMEM((G1, R, 640), F32),
            pltpu.VMEM((G1, R, 640), F32),
            pltpu.VMEM((256, 640), F32),
            pieces(7, 16), pieces(N_SPACE, 16), pieces(G1, 16), pieces(7, 16),
            pltpu.VMEM((RP, 640), F32),
            pltpu.VMEM((G2, R, 256), F32),
            pltpu.VMEM((G2, R, 256), F32),
            pltpu.VMEM((128, 256), F32),
            pieces(5, 8), pieces(N_SPACE, 8), pieces(N_TM, 8), pieces(5, 8),
            pltpu.SemaphoreType.DMA((X_PARTS,)),
            pltpu.SemaphoreType.DMA((N_TM,)),
            pltpu.SemaphoreType.DMA((10,)),
        ],
        compiler_params=pltpu.CompilerParams(collective_id=0, has_side_effects=True),
    )(snapshots, start_block.T, merge_mix.T)
    modes, spectrum = pl.pallas_call(
        write_out,
        out_shape=(jax.ShapeDtypeStruct((R, PIECE), F32), jax.ShapeDtypeStruct((1, R), F32)),
        in_specs=[vmem],
        out_specs=(vmem, vmem),
    )(result)
    return modes, spectrum.reshape(R)


def solution(mesh):
    return jax.shard_map(
        local,
        mesh=mesh,
        in_specs=(P("tm", "space"), P("tm", None), P()),
        out_specs=(P(None, ("space", "tm")), P()),
        check_vma=False,
    )
```
